32 devices in a mesh: tm: 8 (over y, x, core), chan: 4 (over z).
Axes of the slice: x: 2, y: 2, z: 4, core: 2. Of those that a mesh axis runs over, the one named last changes fastest.
Arguments:
- samples: bfloat16 [2, 16384, 2048], P(None, ('tm', 'chan')), may hold values from -6 to 6
- taps: float32 [8, 2048], replicated, may hold values from -2.5 to 2.5
Outputs:
- spectra: bfloat16 [2, 2, 1024, 16384], P(None, None, ('tm', 'chan'))
The draws below stay inside these ranges and needn't reach their ends.
All inputs are finite; a program needn't handle non-finite values.
Results may differ from the reference program's by a relative error of at most 0.0055.
Values may be sent and summed in bfloat16 or wider, within the bound.
No kernel may reach another device: no remote copies, remote signals or barrier semaphores. Data moves between devices by JAX's collectives and lax.ppermute only.
A program may use at most 64 MiB of HBM per device.

```python
import jax
import jax.numpy as jnp
from jax import lax

NFFT = 2048
TAPS = 8
POL = 2
F_DEV = 512
FRAMES = 16384
CHANNELS = 1024


def level_of(key, extent, cuts, low, largest):
    gain, own = 1.0, jax.random.fold_in(key, 6)
    for axis_at, blocks in cuts:
        draws = jnp.exp(jax.random.uniform(jax.random.fold_in(own, axis_at), (blocks,), jnp.float32, low / len(cuts), largest / len(cuts)))
        gain = gain * jnp.repeat(draws, extent[axis_at] // blocks).reshape([-1 if axis == axis_at else 1 for axis in range(len(extent))])
    return gain


def centred(own_key, dims, width, limit, shards=(), kind=jnp.bfloat16):
    entries = jax.random.normal(own_key, dims, jnp.float32) * width
    if len(shards) > 0:
        entries = level_of(own_key, dims, shards, -0.22, 0.18) * entries
    return jnp.clip(entries, min=-limit, max=limit).astype(kind)


def setup_inputs(seed: int = 0) -> dict:
    streams_of = jax.random.split(jax.random.key(seed), 3)
    return {
        "samples": centred(streams_of[0], (POL, FRAMES, NFFT), 1.0, 6.0, ((1, 32),)),
        "taps": centred(streams_of[1], (TAPS, NFFT), 0.35, 2.5, (), jnp.float32),
    }


def make_table(nfft, count):
    index_k = jnp.arange(count, dtype=jnp.int32)[:, None]
    index_n = jnp.arange(nfft, dtype=jnp.int32)[None, :]
    phase = ((index_k * index_n) % nfft).astype(jnp.float32)
    angle = phase * (2.0 * 3.141592653589793 / nfft)
    return jnp.stack([jnp.cos(angle) / 32.0, -jnp.sin(angle) / 32.0]).astype(jnp.bfloat16)


def reference(samples, taps):
    table = make_table(NFFT, CHANNELS).astype(jnp.float32)
    padded = jnp.concatenate([jnp.zeros((POL, TAPS - 1, NFFT), samples.dtype), samples], axis=1)
    blocks = FRAMES // F_DEV

    def one_block(block):
        start = (block * F_DEV).astype(jnp.int32)
        window = lax.dynamic_slice_in_dim(padded, start, F_DEV + TAPS - 1, 1).astype(jnp.float32)
        weighted = jnp.zeros((POL, F_DEV, NFFT), jnp.float32)
        for tap in range(TAPS):
            weighted = weighted + taps[tap][None, None, :] * window[:, tap:tap + F_DEV, :]
        weighted = weighted.astype(jnp.bfloat16).astype(jnp.float32)
        return jnp.einsum('ckn,pfn->cpkf', table, weighted).astype(jnp.bfloat16)

    pieces = lax.map(one_block, jnp.arange(blocks, dtype=jnp.int32))
    pieces = jnp.transpose(pieces, (1, 2, 3, 0, 4))
    return pieces.reshape(2, POL, CHANNELS, FRAMES)
```

```python
import functools

import jax
import jax.numpy as jnp
import numpy as np
from jax import lax
from jax.experimental import pallas as pl
from jax.experimental.pallas import tpu as pltpu
from jax.sharding import PartitionSpec as P


LANES = 128
ROWS = 8
VMEM_LIMIT = 60 * 1024 * 1024


def axis_moves(count):
    if count & (count - 1) == 0:
        return [(lambda i, d=d: i ^ d) for d in range(count)], [(lambda i, d=d: i ^ d) for d in range(count)]
    to = [(lambda i, d=d: (i + d) % count) for d in range(count)]
    back = [(lambda i, d=d: (i + count - d) % count) for d in range(count)]
    return to, back


def twiddles(nfft):
    span = nfft // LANES
    high = np.arange(nfft // 2 // span)[:, None] * span * np.arange(LANES)[None, :]
    low = np.arange(span)[:, None] * np.arange(LANES)[None, :]
    step = np.arange(span)[:, None] * np.arange(span)[None, :] * LANES

    def pair(turns):
        angle = 2.0 * np.pi * (turns % nfft) / nfft
        return np.stack([np.cos(angle), np.sin(angle)]).astype(np.float32)

    step = np.broadcast_to(pair(step)[:, :, :, None] / 32.0, (2, span, span, LANES))
    return jnp.asarray(pair(high)), jnp.asarray(pair(low)), jnp.asarray(np.ascontiguousarray(step))


def fir(samples_ref, halo_ref, taps_ref, weighted_ref, ext_ref):
    pols, frames, nfft = samples_ref.shape
    tap_count = taps_ref.shape[0]
    chunks = nfft // LANES

    def body(step, carry):
        pol = step // chunks
        at = pl.ds(pl.multiple_of(step % chunks * LANES, LANES), LANES)
        ext_ref[pl.ds(0, ROWS), :] = halo_ref[pol, :, at].astype(jnp.float32)
        ext_ref[pl.ds(ROWS, frames), :] = samples_ref[pol, :, at].astype(jnp.float32)
        taps = taps_ref[:, at]
        rows = 64
        for first in range(0, frames, rows):
            total = None
            for tap in range(tap_count):
                start = ROWS + first + tap - (tap_count - 1)
                term = taps[tap : tap + 1, :] * ext_ref[pl.ds(start, rows), :]
                total = term if total is None else total + term
            weighted_ref[pol, pl.ds(first, rows), at] = total.astype(jnp.bfloat16)
        return carry

    lax.fori_loop(0, pols * chunks, body, 0)


def fill_phases(high_ref, low_ref, phase_ref):
    span = low_ref.shape[1]
    for a in range(high_ref.shape[1]):
        high_c, high_s = high_ref[0, pl.ds(a, 1), :], high_ref[1, pl.ds(a, 1), :]
        low_c, low_s = low_ref[0], low_ref[1]
        phase_ref[0, pl.ds(a * span, span), :] = high_c * low_c - high_s * low_s
        phase_ref[1, pl.ds(a * span, span), :] = high_s * low_c + high_c * low_s


def fill_table(dest, slot, own, phase_ref, step_ref, table_ref):
    span = step_ref.shape[1]
    for first in range(0, own, ROWS):
        k = pl.multiple_of(dest * own + first, ROWS)
        c, s = phase_ref[0, pl.ds(k, ROWS), :], phase_ref[1, pl.ds(k, ROWS), :]
        r = pl.multiple_of(lax.rem(k, span), ROWS)
        at_c = slot * 2 * own + first
        at_s = at_c + own
        for m in range(span):
            mc, ms = step_ref[0, m, pl.ds(r, ROWS), :], step_ref[1, m, pl.ds(r, ROWS), :]
            lanes = pl.ds(m * LANES, LANES)
            table_ref[pl.ds(at_c, ROWS), lanes] = (c * mc - s * ms).astype(jnp.bfloat16)
            table_ref[pl.ds(at_s, ROWS), lanes] = (-(s * mc + c * ms)).astype(jnp.bfloat16)


def transform(dests, out_refs, own, weighted_ref, phase_ref, step_ref, table_ref):
    pols, frames, _ = weighted_ref.shape
    per = table_ref.shape[0] // (2 * own)
    wide = 256
    for first in range(0, len(dests), per):
        group = dests[first : first + per]
        outs = out_refs[first : first + per]
        for slot, dest in enumerate(group):
            fill_table(dest, slot, own, phase_ref, step_ref, table_ref)
        rows = len(group) * 2 * own

        for pol in range(pols):

            def body(step, carry, pol=pol, rows=rows, outs=outs):
                at = pl.ds(pl.multiple_of(step * wide, wide), wide)
                part = lax.dot_general(
                    table_ref[pl.ds(0, rows), :],
                    weighted_ref[pol, at, :],
                    (((1,), (1,)), ((), ())),
                    preferred_element_type=jnp.float32,
                ).astype(jnp.bfloat16)
                for slot, out in enumerate(outs):
                    for c in range(2):
                        row = (slot * 2 + c) * own
                        out[c, pol, :, at] = part[row : row + own]
                return carry

            lax.fori_loop(0, frames // wide, body, 0)


def destination(axes, move):
    rows, columns = axes
    (to_row, to_column) = move
    return to_row(lax.axis_index(rows[0])) * columns[1] + to_column(lax.axis_index(columns[0]))


def first_kernel(axes, moves, own, samples, halo, taps, high, low, step, weighted, *refs):
    outs, (ext, phase, table) = refs[: len(moves)], refs[len(moves) :]
    fir(samples, halo, taps, weighted, ext)
    fill_phases(high, low, phase)
    dests = [destination(axes, move) for move in moves]
    transform(dests, outs, own, weighted, phase, step, table)


def rest_kernel(axes, moves, own, weighted, high, low, step, *refs):
    outs, (phase, table) = refs[: len(moves)], refs[len(moves) :]
    fill_phases(high, low, phase)
    dests = [destination(axes, move) for move in moves]
    transform(dests, outs, own, weighted, phase, step, table)


def place_kernel(axes, moves, frames, *refs):
    blocks, out, sems = refs[: len(moves)], refs[len(moves)], refs[len(moves) + 1]
    copies = []
    for i, (block, move) in enumerate(zip(blocks, moves)):
        at = pl.ds(pl.multiple_of(destination(axes, move) * frames, LANES), frames)
        copies.append(pltpu.make_async_copy(block, out.at[:, :, :, at], sems.at[i]))
    for copy in copies:
        copy.start()
    for copy in copies:
        copy.wait()


def local(axes, samples, taps):
    (row_axis, row_count), (column_axis, column_count) = axes
    pols, frames, nfft = samples.shape
    tap_count = taps.shape[0]
    channels = nfft // 2
    devices = row_count * column_count
    own = channels // devices
    assert own % ROWS == 0 and tap_count <= ROWS and nfft % LANES == 0 and frames % 256 == 0

    both = (row_axis, column_axis)
    tail = samples[:, frames - ROWS :, :]
    halo = lax.ppermute(tail, both, [(i, i + 1) for i in range(devices - 1)])

    row_to, row_back = axis_moves(row_count)
    column_to, column_back = axis_moves(column_count)
    order = [(r, c) for c in reversed(range(column_count)) for r in range(row_count)]
    sends = [(row_to[r], column_to[c]) for r, c in order]
    comes = [(row_back[r], column_back[c]) for r, c in order]

    per = max(1, 256 // (2 * own))
    high, low, step = twiddles(nfft)
    block = jax.ShapeDtypeStruct((2, pols, own, frames), jnp.bfloat16)
    vmem = pl.BlockSpec(memory_space=pltpu.VMEM)
    span = nfft // LANES
    scratch = [pltpu.VMEM((2, channels, LANES), jnp.float32), pltpu.VMEM((per * 2 * own, nfft), jnp.bfloat16)]

    def cost(count):
        return pl.CostEstimate(
            flops=2 * count * 2 * own * pols * frames * nfft, bytes_accessed=2 * pols * frames * nfft * 2, transcendentals=0
        )

    with jax.named_scope("first"):
        weighted, *ready = pl.pallas_call(
            functools.partial(first_kernel, axes, sends[:per], own),
            out_shape=[jax.ShapeDtypeStruct(samples.shape, jnp.bfloat16)] + [block] * per,
            in_specs=[vmem] * 6,
            out_specs=[vmem] * (1 + per),
            scratch_shapes=[pltpu.VMEM((frames + ROWS, LANES), jnp.float32)] + scratch,
            compiler_params=pltpu.CompilerParams(vmem_limit_bytes=VMEM_LIMIT),
            cost_estimate=cost(per),
            name="first",
        )(samples, halo, taps, high, low, step)
    with jax.named_scope("rest"):
        rest = pl.pallas_call(
            functools.partial(rest_kernel, axes, sends[per:], own),
            out_shape=[block] * (devices - per),
            in_specs=[vmem] * 4,
            out_specs=[vmem] * (devices - per),
            scratch_shapes=scratch,
            compiler_params=pltpu.CompilerParams(vmem_limit_bytes=VMEM_LIMIT),
            cost_estimate=cost(devices - per),
            name="rest",
        )(weighted, high, low, step)

    arrived = []
    for (r, c), part in zip(order, [*ready, *rest]):
        if (r, c) == (0, 0):
            arrived.append(part)
            continue
        pairs = [
            (i * column_count + j, row_to[r](i) * column_count + column_to[c](j))
            for i in range(row_count)
            for j in range(column_count)
        ]
        arrived.append(lax.ppermute(part, both, pairs))

    with jax.named_scope("place"):
        return pl.pallas_call(
            functools.partial(place_kernel, axes, comes, frames),
            out_shape=jax.ShapeDtypeStruct((2, pols, own, devices * frames), jnp.bfloat16),
            in_specs=[pl.BlockSpec(memory_space=pl.ANY)] * devices,
            out_specs=pl.BlockSpec(memory_space=pl.ANY),
            scratch_shapes=[pltpu.SemaphoreType.DMA((devices,))],
            compiler_params=pltpu.CompilerParams(vmem_limit_bytes=1024 * 1024),
            name="place",
        )(*arrived)


def solution(mesh):
    axes = tuple((name, mesh.shape[name]) for name in ("tm", "chan"))
    return jax.shard_map(
        functools.partial(local, axes),
        mesh=mesh,
        in_specs=(P(None, ("tm", "chan"), None), P()),
        out_specs=P(None, None, ("tm", "chan"), None),
        check_vma=False,
    )
```

```python
import functools

import jax
import jax.numpy as jnp
import numpy as np
from jax import lax
from jax.experimental import pallas as pl
from jax.experimental.pallas import tpu as pltpu
from jax.sharding import PartitionSpec as P


LANES = 128
ROWS = 8
CHUNK = 128
PIECES = 4
LEAD = 1
VMEM_LIMIT = 60 * 1024 * 1024


def twiddles(nfft):
    span = nfft // LANES
    high = np.arange(nfft // 2 // span)[:, None] * span * np.arange(LANES)[None, :]
    low = np.arange(span)[:, None] * np.arange(LANES)[None, :]
    step = np.arange(span)[:, None] * np.arange(span)[None, :] * LANES

    def pair(turns):
        angle = 2.0 * np.pi * (turns % nfft) / nfft
        return np.stack([np.cos(angle), np.sin(angle)]).astype(np.float32)

    step = np.broadcast_to(pair(step)[:, :, :, None] / 32.0, (2, span, span, LANES))
    return jnp.asarray(pair(high)), jnp.asarray(pair(low)), jnp.asarray(np.ascontiguousarray(step))


def fir(load, chunks, taps_ref, weighted_ref, ext_ref):
    nfft = taps_ref.shape[1]
    tap_count = taps_ref.shape[0]
    pols = weighted_ref.shape[1] // CHUNK

    def body(step, carry):
        pol = lax.rem(step, pols)
        at = pl.ds(pl.multiple_of(step // pols * LANES, LANES), LANES)
        load(step, pol, at)
        taps = taps_ref[:, at]
        rows = 64
        for chunk in range(chunks):
            for first in range(0, CHUNK, rows):
                total = None
                for tap in range(tap_count):
                    start = ROWS + chunk * CHUNK + first + tap - (tap_count - 1)
                    term = taps[tap : tap + 1, :] * ext_ref[pl.ds(start, rows), :]
                    total = term if total is None else total + term
                to = pl.ds(pl.multiple_of(pol * CHUNK + first, rows), rows)
                weighted_ref[chunk, to, at] = total.astype(jnp.bfloat16)
        return carry

    lax.fori_loop(0, pols * nfft // LANES, body, 0)


def fill_phases(high_ref, low_ref, phase_ref):
    span = low_ref.shape[1]
    for a in range(high_ref.shape[1]):
        high_c, high_s = high_ref[0, pl.ds(a, 1), :], high_ref[1, pl.ds(a, 1), :]
        low_c, low_s = low_ref[0], low_ref[1]
        phase_ref[0, pl.ds(a * span, span), :] = high_c * low_c - high_s * low_s
        phase_ref[1, pl.ds(a * span, span), :] = -(high_s * low_c) - high_c * low_s


def fill_table(group, dest_of, own, phase_ref, step_ref, table_ref):
    span = step_ref.shape[1]
    height = 2 * ROWS if own % (2 * ROWS) == 0 and span % (2 * ROWS) == 0 else ROWS
    per = table_ref.shape[0] // (2 * own)
    for slot in range(per):
        for first in range(0, own, height):
            k = pl.multiple_of(dest_of(group * per + slot) * own + first, height)
            c, s = phase_ref[0, pl.ds(k, height), :], phase_ref[1, pl.ds(k, height), :]
            r = 0 if height == span else pl.multiple_of(lax.rem(k, span), height)
            at_c = slot * 2 * own + first
            at_s = at_c + own
            for m in range(span):
                mc, ms = step_ref[0, m, pl.ds(r, height), :], step_ref[1, m, pl.ds(r, height), :]
                lanes = pl.ds(m * LANES, LANES)
                table_ref[pl.ds(at_c, height), lanes] = (c * mc + s * ms).astype(jnp.bfloat16)
                table_ref[pl.ds(at_s, height), lanes] = (s * mc - c * ms).astype(jnp.bfloat16)


def transform(store, count, dest_of, own, weighted_ref, phase_ref, step_ref, table_refs):
    per = table_refs[0].shape[0] // (2 * own)
    groups = count // per

    def one(group, now, later):
        for chunk in range(weighted_ref.shape[0]):
            part = lax.dot_general(
                now[...],
                weighted_ref[chunk],
                (((1,), (1,)), ((), ())),
                preferred_element_type=jnp.float32,
            ).astype(jnp.bfloat16)
            for slot in range(per):
                for c in range(2):
                    row = (slot * 2 + c) * own
                    store(group * per + slot, c, chunk, part[row : row + own])
            if chunk == 0:
                fill_table(jnp.minimum(group + 1, groups - 1), dest_of, own, phase_ref, step_ref, later)

    def two(index, carry):
        one(2 * index, table_refs[0], table_refs[1])
        one(2 * index + 1, table_refs[1], table_refs[0])
        return carry

    lax.fori_loop(0, groups // 2, two, 0)
    if groups % 2:
        one(groups - 1, table_refs[0], table_refs[1])


def position(axes):
    return lax.axis_index(axes[0][0]) * axes[1][1] + lax.axis_index(axes[1][0])


def within(axes, item):
    half = axes[1][1] // 2
    return item // half * axes[1][1] + item % half


def compute_kernel(axes, kind, begin, own, samples, *refs):
    refs = list(refs)
    halo = refs.pop(0) if kind == "all" else None
    brought = refs.pop(0) if kind == "near" else None
    taps, high, low, step, out = refs[:5]
    rows, weighted, ext, phase, table, table_next, sems = refs[-7:]
    pols, _, nfft = samples.shape
    count = weighted.shape[0] * CHUNK
    pieces = sems.shape[0]
    wide = nfft // pieces
    first = 0 if halo is not None else begin - ROWS
    held = begin + count - first
    copies = [
        pltpu.make_async_copy(
            samples.at[:, pl.ds(first, held), pl.ds(piece * wide, wide)],
            rows.at[:, :, pl.ds(piece * wide, wide)],
            sems.at[piece],
        )
        for piece in range(pieces)
    ]
    for copy in copies:
        copy.start()

    half = axes[1][1] // 2
    if kind == "all":
        dest_of = lambda item: item
    else:
        me = position(axes)
        dest_of = lambda item: me ^ (within(axes, item) + (half if kind == "far" else 0))

    def store(item, c, chunk, part):
        for pol in range(pols):
            block = part[:, pol * CHUNK : (pol + 1) * CHUNK]
            if kind == "near":
                out[item, 0, c, pol] = block
            else:
                out[item, c, pol, :, pl.ds(chunk * CHUNK, CHUNK)] = block

    fill_phases(high, low, phase)
    fill_table(0, dest_of, own, phase, step, table)
    steps = wide // LANES * pols

    def load(at_step, pol, at):
        for piece, copy in enumerate(copies):
            pl.when(at_step == piece * steps)(copy.wait)
        if halo is not None:
            ext[pl.ds(0, ROWS), :] = halo[pol, :, at].astype(jnp.float32)
            ext[pl.ds(ROWS, held), :] = rows[pol, :, at].astype(jnp.float32)
        else:
            ext[...] = rows[pol, :, at].astype(jnp.float32)

    fir(load, count // CHUNK, taps, weighted, ext)
    transform(store, out.shape[0], dest_of, own, weighted, phase, step, (table, table_next))
    if kind == "near":

        def hand_on(item, carry):
            out[item, 1] = brought[item]
            return carry

        lax.fori_loop(0, out.shape[0], hand_on, 0)


def place_main_kernel(frames, block, held, out, sems):
    copies = []
    for source in range(block.shape[0]):
        at = pl.ds(source * frames, block.shape[4])
        copies.append(pltpu.make_async_copy(block.at[source], out.at[:, :, :, at], sems.at[source]))
    for copy in copies:
        copy.start()
    for copy in copies:
        copy.wait()


def place_near_kernel(axes, frames, begin, *refs):
    blocks, (mine, out, sems) = refs[:-3], refs[-3:]
    half = axes[1][1] // 2
    me = position(axes)
    copies = []
    for item in range(len(blocks) + 1):
        block = mine if item == 0 else blocks[item - 1]
        for side in range(2):
            source = me ^ (within(axes, item) + side * half)
            at = pl.ds(pl.multiple_of(source * frames + begin, CHUNK), frames - begin)
            copies.append(pltpu.make_async_copy(block.at[side], out.at[:, :, :, at], sems.at[2 * item + side]))
    for copy in copies:
        copy.start()
    for copy in copies:
        copy.wait()


def local(axes, samples, taps):
    pols, frames, nfft = samples.shape
    tap_count = taps.shape[0]
    channels = nfft // 2
    both = tuple(name for name, _ in axes)
    row_count, column_count = axes[0][1], axes[1][1]
    devices = row_count * column_count
    half = column_count // 2
    own = channels // devices
    chunks = frames // CHUNK
    per = max(1, 256 // (2 * own))
    assert own % ROWS == 0 and tap_count <= ROWS and nfft % (LANES * PIECES) == 0 and frames % CHUNK == 0 and chunks > 1
    assert devices & (devices - 1) == 0 and half > 0 and row_count * half % per == 0

    high, low, step = twiddles(nfft)
    bf16 = jnp.bfloat16
    vmem = pl.BlockSpec(memory_space=pltpu.VMEM)
    anywhere = pl.BlockSpec(memory_space=pl.ANY)
    dma = pltpu.SemaphoreType.DMA
    nears = row_count * half
    begin = (chunks - LEAD) * CHUNK
    short = frames - begin

    def compute(kind, at, count, out_shape, *extra):
        held = count * CHUNK + (0 if kind == "all" else ROWS)
        dests = devices if kind == "all" else nears
        return pl.pallas_call(
            functools.partial(compute_kernel, axes, kind, at, own),
            out_shape=[jax.ShapeDtypeStruct(shape, bf16) for shape in out_shape],
            in_specs=[anywhere] + [vmem] * (4 + len(extra)),
            out_specs=[vmem] * len(out_shape),
            scratch_shapes=[
                pltpu.VMEM((pols, held, nfft), bf16),
                pltpu.VMEM((count, pols * CHUNK, nfft), bf16),
                pltpu.VMEM((count * CHUNK + ROWS, LANES), jnp.float32),
                pltpu.VMEM((2, channels, LANES), jnp.float32),
                pltpu.VMEM((per * 2 * own, nfft), bf16),
                pltpu.VMEM((per * 2 * own, nfft), bf16),
                dma((PIECES,)),
            ],
            compiler_params=pltpu.CompilerParams(vmem_limit_bytes=VMEM_LIMIT),
            cost_estimate=pl.CostEstimate(
                flops=4 * dests * own * pols * count * CHUNK * nfft,
                bytes_accessed=2 * pols * count * CHUNK * nfft * 2,
                transcendentals=0,
            ),
        )(samples, *extra, taps, high, low, step)

    def swap(part, by):
        return lax.ppermute(part, both, [(i, i ^ by) for i in range(devices)])

    out_shape = jax.ShapeDtypeStruct((2, pols, own, devices * frames), bf16)
    small = pltpu.CompilerParams(vmem_limit_bytes=1024 * 1024)

    halo = lax.ppermute(samples[:, frames - ROWS :, :], both, [(i, i + 1) for i in range(devices - 1)])
    (part,) = compute("far", begin, LEAD, [(nears, 2, pols, own, short)])
    brought = swap(part, half)
    (part,) = compute("all", 0, chunks - LEAD, [(devices, 2, pols, own, begin)], halo)
    arrived = lax.all_to_all(part, both, split_axis=0, concat_axis=0, tiled=True)
    (part,) = compute("near", begin, LEAD, [(nears, 2, 2, pols, own, short)], brought)
    blocks = [swap(part[item], item // half * column_count + item % half) for item in range(1, nears)]
    out = pl.pallas_call(
        functools.partial(place_near_kernel, axes, frames, begin),
        out_shape=out_shape,
        in_specs=[anywhere] * (nears - 1) + [vmem],
        out_specs=anywhere,
        scratch_shapes=[dma((2 * nears,))],
        compiler_params=small,
        name="place_near",
    )(*blocks, part[0])
    return pl.pallas_call(
        functools.partial(place_main_kernel, frames),
        out_shape=out_shape,
        in_specs=[anywhere] * 2,
        out_specs=anywhere,
        scratch_shapes=[dma((devices,))],
        input_output_aliases={1: 0},
        compiler_params=small,
        name="place_main",
    )(arrived, out)


def solution(mesh):
    axes = tuple((name, mesh.shape[name]) for name in ("tm", "chan"))

    def body(samples, taps):
        return local(axes, samples, taps)

    return jax.shard_map(
        body,
        mesh=mesh,
        in_specs=(P(None, ("tm", "chan"), None), P()),
        out_specs=P(None, None, ("tm", "chan"), None),
        check_vma=False,
    )
```

```python
import functools

import jax
import jax.numpy as jnp
import numpy as np
from jax import lax
from jax.experimental import pallas as pl
from jax.experimental.pallas import tpu as pltpu
from jax.sharding import PartitionSpec as P


LANES = 128
ROWS = 8
CHUNK = 128
PIECES = 4
LEAD = 1
VMEM_LIMIT = 60 * 1024 * 1024


def twiddles(nfft, radix):
    span = nfft // LANES
    r = np.arange(span).reshape(-1, radix).T.reshape(-1)
    high = np.arange(nfft // 2 // span)[:, None] * span * np.arange(LANES)[None, :]
    low = r[:, None] * np.arange(LANES)[None, :]
    step = np.arange(span // radix)[:, None] * r[None, :] * LANES

    def pair(turns):
        angle = 2.0 * np.pi * (turns % nfft) / nfft
        return np.stack([np.cos(angle), np.sin(angle)]).astype(np.float32)

    step = np.broadcast_to(pair(step)[:, :, :, None] / 32.0, (2, span // radix, span, LANES))
    return jnp.asarray(pair(high)), jnp.asarray(pair(low)), jnp.asarray(np.ascontiguousarray(step))


def fir(load, chunks, taps_ref, weighted_ref, ext_ref):
    nfft = taps_ref.shape[1]
    tap_count = taps_ref.shape[0]
    radix = weighted_ref.shape[0]
    pols = weighted_ref.shape[2] // CHUNK
    width = nfft // radix
    rows = 64 // radix

    def body(step, carry):
        pol = lax.rem(step, pols)
        lane = pl.multiple_of(step // pols * LANES, LANES)
        taps = []
        for part in range(radix):
            at = pl.ds(lane + part * width, LANES)
            load(step, pol, part, at)
            taps.append(taps_ref[:, at])
        for chunk in range(chunks):
            for first in range(0, CHUNK, rows):
                totals = []
                for part in range(radix):
                    total = None
                    for tap in range(tap_count):
                        start = ROWS + chunk * CHUNK + first + tap - (tap_count - 1)
                        term = taps[part][tap : tap + 1, :] * ext_ref[part, pl.ds(start, rows), :]
                        total = term if total is None else total + term
                    totals.append(total)
                to = pl.ds(pl.multiple_of(pol * CHUNK + first, rows), rows)
                if radix == 2:
                    totals = [totals[0] + totals[1], totals[0] - totals[1]]
                for part in range(radix):
                    weighted_ref[part, chunk, to, pl.ds(lane, LANES)] = totals[part].astype(jnp.bfloat16)
        return carry

    lax.fori_loop(0, pols * width // LANES, body, 0)


def fill_phases(high_ref, low_ref, phase_ref):
    span = low_ref.shape[1]
    for a in range(high_ref.shape[1]):
        high_c, high_s = high_ref[0, pl.ds(a, 1), :], high_ref[1, pl.ds(a, 1), :]
        low_c, low_s = low_ref[0], low_ref[1]
        phase_ref[0, pl.ds(a * span, span), :] = high_c * low_c - high_s * low_s
        phase_ref[1, pl.ds(a * span, span), :] = -(high_s * low_c) - high_c * low_s


def fill_table(group, dest_of, own, phase_ref, step_ref, table_ref):
    radix = table_ref.shape[0]
    steps, span = step_ref.shape[1:3]
    per = table_ref.shape[1] * radix // (2 * own)
    height = min(own, span) // radix
    blocks = own * radix // (height * radix * radix)
    for slot in range(per):
        k = dest_of(group * per + slot) * own
        for part in range(radix):
            at = part * (span // radix)
            inner = 0 if height * radix == span else pl.multiple_of(lax.rem(k, span), ROWS)
            base = pl.multiple_of(k - inner, span)
            joined = lambda pieces: pieces[0] if len(pieces) == 1 else jnp.concatenate(pieces)
            rows = [pl.ds(pl.multiple_of(base + block * span + at + inner, ROWS), height) for block in range(blocks)]
            c = joined([phase_ref[0, r, :] for r in rows])
            s = joined([phase_ref[1, r, :] for r in rows])
            to_c = slot * 2 * own // radix
            to_s = to_c + own // radix
            for m in range(steps):
                of = pl.ds(pl.multiple_of(at + inner, ROWS), height)
                mc = joined([step_ref[0, m, of, :]] * blocks)
                ms = joined([step_ref[1, m, of, :]] * blocks)
                lanes = pl.ds(m * LANES, LANES)
                table_ref[part, pl.ds(to_c, own // radix), lanes] = (c * mc + s * ms).astype(jnp.bfloat16)
                table_ref[part, pl.ds(to_s, own // radix), lanes] = (s * mc - c * ms).astype(jnp.bfloat16)


def transform(store, send, count, dest_of, own, weighted_ref, phase_ref, step_ref, table_refs, mixed_ref):
    radix, rows, _ = table_refs[0].shape
    per = rows * radix // (2 * own)
    groups = count // per

    def one(group, now, later):
        for chunk in range(weighted_ref.shape[1]):
            for part in range(radix):
                found = lax.dot_general(
                    now[part],
                    weighted_ref[part, chunk],
                    (((1,), (1,)), ((), ())),
                    preferred_element_type=jnp.float32,
                )
                for side in range(mixed_ref.shape[0]):
                    to = pl.ds(part, rows, stride=radix) if radix > 1 else pl.ds(0, rows)
                    mixed_ref[side, to, :] = found[:, side * LANES : (side + 1) * LANES]
            for slot in range(per):
                for c in range(2):
                    row = pl.ds((slot * 2 + c) * own, own)
                    store(group * per + slot, c, chunk, [mixed_ref[side, row, :] for side in range(mixed_ref.shape[0])])
            if chunk == 0:
                fill_table(jnp.minimum(group + 1, groups - 1), dest_of, own, phase_ref, step_ref, later)

    def two(index, carry):
        one(2 * index, table_refs[0], table_refs[1])
        one(2 * index + 1, table_refs[1], table_refs[0])
        send(index).start()
        return carry

    lax.fori_loop(0, groups // 2, two, 0)

    def settle(index, carry):
        send(index).wait()
        return carry

    lax.fori_loop(0, groups // 2, settle, 0)


def position(axes):
    return lax.axis_index(axes[0][0]) * axes[1][1] + lax.axis_index(axes[1][0])


def within(axes, item):
    half = axes[1][1] // 2
    return item // half * axes[1][1] + item % half


def compute_kernel(axes, kind, begin, own, samples, *refs):
    refs = list(refs)
    halo = refs.pop(0) if kind == "all" else None
    brought = refs.pop(0) if kind == "near" else None
    result = refs[4]
    rows, weighted, ext, phase, table, table_next, mixed, out, taps, high, low, step, sems, constant_sems, out_sems = refs[5:]
    pols, _, nfft = samples.shape
    radix = weighted.shape[0]
    count = weighted.shape[1] * CHUNK
    pieces = sems.shape[0]
    width = nfft // radix
    wide = width // pieces
    first = 0 if halo is not None else begin - ROWS
    held = begin + count - first
    copies = [
        pltpu.make_async_copy(
            samples.at[:, pl.ds(first, held), pl.ds(part * width + piece * wide, wide)],
            rows.at[:, :, pl.ds(part * width + piece * wide, wide)],
            sems.at[piece, part],
        )
        for piece in range(pieces)
        for part in range(radix)
    ]
    constants = [
        pltpu.make_async_copy(source, to, constant_sems.at[i])
        for i, (source, to) in enumerate(zip(refs[:4], (taps, high, low, step)))
    ]
    for copy in copies + constants:
        copy.start()

    half = axes[1][1] // 2
    if kind == "all":
        dest_of = lambda item: item
    else:
        me = position(axes)
        dest_of = lambda item: me ^ (within(axes, item) + (half if kind == "far" else 0))

    together = result.shape[0] // out_sems.shape[0]

    def send(index):
        items = pl.ds(index * together, together)
        return pltpu.make_async_copy(out.at[items], result.at[items], out_sems.at[index])

    def store(item, c, chunk, part):
        for pol in range(pols):
            block = part[pol].astype(jnp.bfloat16)
            if kind == "near":
                out[item, 0, c, pol] = block
                out[item, 1, c, pol] = brought[item, c, pol]
            else:
                out[item, c, pol, :, pl.ds(chunk * CHUNK, CHUNK)] = block

    for copy in constants:
        copy.wait()
    fill_phases(high, low, phase)
    fill_table(0, dest_of, own, phase, step, table)
    steps = wide // LANES * pols

    def load(at_step, pol, part, at):
        for piece in range(pieces):
            pl.when(at_step == piece * steps)(copies[piece * radix + part].wait)
        if halo is not None:
            ext[part, pl.ds(0, ROWS), :] = halo[pol, :, at].astype(jnp.float32)
            ext[part, pl.ds(ROWS, held), :] = rows[pol, :, at].astype(jnp.float32)
        else:
            ext[part] = rows[pol, :, at].astype(jnp.float32)

    fir(load, count // CHUNK, taps, weighted, ext)
    transform(store, send, out.shape[0], dest_of, own, weighted, phase, step, (table, table_next), mixed)


def place_main_kernel(frames, block, held, out, sems):
    copies = []
    for source in range(block.shape[0]):
        at = pl.ds(source * frames, block.shape[4])
        copies.append(pltpu.make_async_copy(block.at[source], out.at[:, :, :, at], sems.at[source]))
    for copy in copies:
        copy.start()
    for copy in copies:
        copy.wait()


def place_near_kernel(axes, frames, begin, *refs):
    blocks, (mine, out, sems) = refs[:-3], refs[-3:]
    half = axes[1][1] // 2
    me = position(axes)
    copies = []
    for item in range(len(blocks) + 1):
        block = mine if item == 0 else blocks[item - 1]
        for side in range(2):
            source = me ^ (within(axes, item) + side * half)
            at = pl.ds(pl.multiple_of(source * frames + begin, CHUNK), frames - begin)
            copies.append(pltpu.make_async_copy(block.at[side], out.at[:, :, :, at], sems.at[2 * item + side]))
    for copy in copies:
        copy.start()
    for copy in copies:
        copy.wait()


def local(axes, samples, taps):
    pols, frames, nfft = samples.shape
    tap_count = taps.shape[0]
    channels = nfft // 2
    both = tuple(name for name, _ in axes)
    row_count, column_count = axes[0][1], axes[1][1]
    devices = row_count * column_count
    half = column_count // 2
    own = channels // devices
    chunks = frames // CHUNK
    radix = 2 if own % (nfft // LANES) == 0 else 1
    per = max(1, 256 * radix // (2 * own))
    assert own % ROWS == 0 and tap_count <= ROWS and nfft % (LANES * PIECES * radix) == 0 and frames % CHUNK == 0 and chunks > 1
    assert devices & (devices - 1) == 0 and half > 0 and row_count * half % (2 * per) == 0

    high, low, step = twiddles(nfft, radix)
    bf16 = jnp.bfloat16
    vmem = pl.BlockSpec(memory_space=pltpu.VMEM)
    anywhere = pl.BlockSpec(memory_space=pl.ANY)
    hbm = pl.BlockSpec(memory_space=pltpu.HBM)
    dma = pltpu.SemaphoreType.DMA
    nears = row_count * half
    begin = (chunks - LEAD) * CHUNK
    short = frames - begin

    def compute(kind, at, count, shape, *extra):
        held = count * CHUNK + (0 if kind == "all" else ROWS)
        dests = devices if kind == "all" else nears
        return pl.pallas_call(
            functools.partial(compute_kernel, axes, kind, at, own),
            out_shape=jax.ShapeDtypeStruct(shape, bf16),
            in_specs=[hbm] + [vmem] * len(extra) + [hbm] * 4,
            out_specs=hbm,
            scratch_shapes=[
                pltpu.VMEM((pols, held, nfft), bf16),
                pltpu.VMEM((radix, count, pols * CHUNK, nfft // radix), bf16),
                pltpu.VMEM((radix, count * CHUNK + ROWS, LANES), jnp.float32),
                pltpu.VMEM((2, channels, LANES), jnp.float32),
                pltpu.VMEM((radix, per * 2 * own // radix, nfft // radix), bf16),
                pltpu.VMEM((radix, per * 2 * own // radix, nfft // radix), bf16),
                pltpu.VMEM((pols * CHUNK // LANES, per * 2 * own, LANES), jnp.float32),
                pltpu.VMEM(shape, bf16),
                pltpu.VMEM(taps.shape, taps.dtype),
                *(pltpu.VMEM(factor.shape, factor.dtype) for factor in (high, low, step)),
                dma((PIECES, radix)),
                dma((4,)),
                dma((dests // (2 * per),)),
            ],
            compiler_params=pltpu.CompilerParams(vmem_limit_bytes=VMEM_LIMIT),
            cost_estimate=pl.CostEstimate(
                flops=4 * dests * own * pols * count * CHUNK * nfft,
                bytes_accessed=2 * pols * count * CHUNK * nfft * 2,
                transcendentals=0,
            ),
        )(samples, *extra, taps, high, low, step)

    def swap(part, by):
        return lax.ppermute(part, both, [(i, i ^ by) for i in range(devices)])

    out_shape = jax.ShapeDtypeStruct((2, pols, own, devices * frames), bf16)
    small = pltpu.CompilerParams(vmem_limit_bytes=1024 * 1024)

    halo = lax.ppermute(samples[:, frames - ROWS :, :], both, [(i, i + 1) for i in range(devices - 1)])
    part = compute("far", begin, LEAD, (nears, 2, pols, own, short))
    brought = swap(part, half)
    part = compute("all", 0, chunks - LEAD, (devices, 2, pols, own, begin), halo)
    arrived = lax.all_to_all(part, both, split_axis=0, concat_axis=0, tiled=True)
    part = compute("near", begin, LEAD, (nears, 2, 2, pols, own, short), brought)
    blocks = [swap(part[item], item // half * column_count + item % half) for item in range(1, nears)]
    out = pl.pallas_call(
        functools.partial(place_near_kernel, axes, frames, begin),
        out_shape=out_shape,
        in_specs=[anywhere] * (nears - 1) + [vmem],
        out_specs=anywhere,
        scratch_shapes=[dma((2 * nears,))],
        compiler_params=small,
        name="place_near",
    )(*blocks, part[0])
    return pl.pallas_call(
        functools.partial(place_main_kernel, frames),
        out_shape=out_shape,
        in_specs=[anywhere] * 2,
        out_specs=anywhere,
        scratch_shapes=[dma((devices,))],
        input_output_aliases={1: 0},
        compiler_params=small,
        name="place_main",
    )(arrived, out)


def solution(mesh):
    axes = tuple((name, mesh.shape[name]) for name in ("tm", "chan"))

    def body(samples, taps):
        return local(axes, samples, taps)

    return jax.shard_map(
        body,
        mesh=mesh,
        in_specs=(P(None, ("tm", "chan"), None), P()),
        out_specs=P(None, None, ("tm", "chan"), None),
        check_vma=False,
    )
```

```python
import functools

import jax
import jax.numpy as jnp
import numpy as np
from jax import lax
from jax.experimental import pallas as pl
from jax.experimental.pallas import tpu as pltpu
from jax.sharding import PartitionSpec as P


LANES = 128
ROWS = 8
CHUNK = 128
PIECES = 4
LEAD = 1
VMEM_LIMIT = 24 * 1024 * 1024


def twiddles(nfft, radix):
    span = nfft // LANES
    r = np.arange(span).reshape(-1, radix).T.reshape(-1)
    high = np.arange(nfft // 2 // span)[:, None] * span * np.arange(LANES)[None, :]
    low = r[:, None] * np.arange(LANES)[None, :]
    step = np.arange(span // radix)[:, None] * r[None, :] * LANES

    def pair(turns):
        angle = 2.0 * np.pi * (turns % nfft) / nfft
        return np.stack([np.cos(angle), np.sin(angle)]).astype(np.float32)

    step = np.broadcast_to(pair(step)[:, :, :, None] / 32.0, (2, span // radix, span, LANES))
    return jnp.asarray(pair(high)), jnp.asarray(pair(low)), jnp.asarray(np.ascontiguousarray(step))


def fir(load, chunks, taps_ref, weighted_ref, ext_ref):
    nfft = taps_ref.shape[1]
    tap_count = taps_ref.shape[0]
    radix = weighted_ref.shape[0]
    pols = weighted_ref.shape[2] // CHUNK
    width = nfft // radix
    rows = 64 // radix

    def body(step, carry):
        pol = lax.rem(step, pols)
        lane = pl.multiple_of(step // pols * LANES, LANES)
        taps = []
        for part in range(radix):
            at = pl.ds(lane + part * width, LANES)
            load(step, pol, part, at)
            taps.append(taps_ref[:, at])
        for chunk in range(chunks):
            for first in range(0, CHUNK, rows):
                totals = []
                for part in range(radix):
                    total = None
                    for tap in range(tap_count):
                        start = ROWS + chunk * CHUNK + first + tap - (tap_count - 1)
                        term = taps[part][tap : tap + 1, :] * ext_ref[part, pl.ds(start, rows), :]
                        total = term if total is None else total + term
                    totals.append(total)
                to = pl.ds(pl.multiple_of(pol * CHUNK + first, rows), rows)
                if radix == 2:
                    totals = [totals[0] + totals[1], totals[0] - totals[1]]
                for part in range(radix):
                    weighted_ref[part, chunk, to, pl.ds(lane, LANES)] = totals[part].astype(jnp.bfloat16)
        return carry

    lax.fori_loop(0, pols * width // LANES, body, 0)


def fill_phases(high_ref, low_ref, phase_ref):
    span = low_ref.shape[1]
    for a in range(high_ref.shape[1]):
        high_c, high_s = high_ref[0, pl.ds(a, 1), :], high_ref[1, pl.ds(a, 1), :]
        low_c, low_s = low_ref[0], low_ref[1]
        phase_ref[0, pl.ds(a * span, span), :] = high_c * low_c - high_s * low_s
        phase_ref[1, pl.ds(a * span, span), :] = -(high_s * low_c) - high_c * low_s


def fill_table(group, dest_of, own, phase_ref, step_ref, table_ref):
    radix = table_ref.shape[0]
    steps, span = step_ref.shape[1:3]
    per = table_ref.shape[1] * radix // (2 * own)
    height = min(own, span) // radix
    blocks = own * radix // (height * radix * radix)
    for slot in range(per):
        k = dest_of(group * per + slot) * own
        for part in range(radix):
            at = part * (span // radix)
            inner = 0 if height * radix == span else pl.multiple_of(lax.rem(k, span), ROWS)
            base = pl.multiple_of(k - inner, span)
            joined = lambda pieces: pieces[0] if len(pieces) == 1 else jnp.concatenate(pieces)
            rows = [pl.ds(pl.multiple_of(base + block * span + at + inner, ROWS), height) for block in range(blocks)]
            c = joined([phase_ref[0, r, :] for r in rows])
            s = joined([phase_ref[1, r, :] for r in rows])
            to_c = slot * 2 * own // radix
            to_s = to_c + own // radix
            for m in range(steps):
                of = pl.ds(pl.multiple_of(at + inner, ROWS), height)
                mc = joined([step_ref[0, m, of, :]] * blocks)
                ms = joined([step_ref[1, m, of, :]] * blocks)
                lanes = pl.ds(m * LANES, LANES)
                table_ref[part, pl.ds(to_c, own // radix), lanes] = (c * mc + s * ms).astype(jnp.bfloat16)
                table_ref[part, pl.ds(to_s, own // radix), lanes] = (s * mc - c * ms).astype(jnp.bfloat16)


def transform(store, count, dest_of, own, weighted_ref, phase_ref, step_ref, table_refs, mixed_ref):
    radix, rows, _ = table_refs[0].shape
    per = rows * radix // (2 * own)
    groups = count // per

    def one(group, now, later):
        for chunk in range(weighted_ref.shape[1]):
            for part in range(radix):
                found = lax.dot_general(
                    now[part],
                    weighted_ref[part, chunk],
                    (((1,), (1,)), ((), ())),
                    preferred_element_type=jnp.float32,
                )
                for side in range(mixed_ref.shape[0]):
                    to = pl.ds(part, rows, stride=radix) if radix > 1 else pl.ds(0, rows)
                    mixed_ref[side, to, :] = found[:, side * LANES : (side + 1) * LANES]
            for slot in range(per):
                for c in range(2):
                    row = pl.ds((slot * 2 + c) * own, own)
                    store(group * per + slot, c, chunk, [mixed_ref[side, row, :] for side in range(mixed_ref.shape[0])])
            if chunk == 0 and later is not None:
                fill_table(jnp.minimum(group + 1, groups - 1), dest_of, own, phase_ref, step_ref, later)

    def two(index, carry):
        one(2 * index, table_refs[0], table_refs[1])
        one(2 * index + 1, table_refs[1], table_refs[0])
        return carry

    if groups == 2:
        one(0, table_refs[0], table_refs[1])
        one(1, table_refs[1], None)
    else:
        lax.fori_loop(0, groups // 2, two, 0)


def position(axes):
    return lax.axis_index(axes[0][0]) * axes[1][1] + lax.axis_index(axes[1][0])


def within(axes, item):
    half = axes[1][1] // 2
    return item // half * axes[1][1] + item % half


def prepare_kernel(axes, begin, own, samples, taps, high, low, step, *refs):
    tail, rows, taps_out, step_out, phase, table, high_in, low_in, sems = refs
    frames = samples.shape[1]
    last = pl.ds(begin - ROWS, frames - begin + ROWS)
    moves = [
        (high, high_in),
        (low, low_in),
        (step, step_out),
        (samples.at[:, pl.ds(frames - ROWS, ROWS)], tail),
        (samples.at[:, last], rows),
        (taps, taps_out),
    ]
    copies = [pltpu.make_async_copy(source, to, sems.at[i]) for i, (source, to) in enumerate(moves)]
    for copy in copies:
        copy.start()
    for copy in copies[:3]:
        copy.wait()
    fill_phases(high_in, low_in, phase)
    me = position(axes)
    fill_table(0, lambda item: me ^ (within(axes, item) + axes[1][1] // 2), own, phase, step_out, table)
    for copy in copies[3:]:
        copy.wait()


def far_kernel(axes, own, rows, taps, step, phase, table, out, weighted, ext, table_next, table_spare, mixed):
    me = position(axes)
    dest_of = lambda item: me ^ (within(axes, item) + axes[1][1] // 2)

    def load(at_step, pol, part, at):
        ext[part] = rows[pol, :, at].astype(jnp.float32)

    def store(item, c, chunk, part):
        for pol in range(out.shape[2]):
            out[item, c, pol, :, pl.ds(chunk * CHUNK, CHUNK)] = part[pol].astype(jnp.bfloat16)

    fir(load, weighted.shape[1], taps, weighted, ext)
    radix, height, _ = table.shape
    first = table
    if out.shape[0] != 2 * (height * radix // (2 * own)):
        table_spare[...] = table[...]
        first = table_spare
    transform(store, out.shape[0], dest_of, own, weighted, phase, step, (first, table_next), mixed)


def compute_kernel(axes, kind, begin, own, samples, *refs):
    refs = list(refs)
    halo = refs.pop(0) if kind == "all" else None
    brought = refs.pop(0) if kind == "near" else None
    out = refs[4]
    rows, weighted, ext, phase, table, table_next, mixed, taps, high, low, step, sems, constant_sems = refs[5:]
    pols, _, nfft = samples.shape
    radix = weighted.shape[0]
    count = weighted.shape[1] * CHUNK
    pieces = sems.shape[0]
    width = nfft // radix
    wide = width // pieces
    first = 0 if halo is not None else begin - ROWS
    held = begin + count - first
    copies = [
        pltpu.make_async_copy(
            samples.at[:, pl.ds(first, held), pl.ds(part * width + piece * wide, wide)],
            rows.at[:, :, pl.ds(part * width + piece * wide, wide)],
            sems.at[piece, part],
        )
        for piece in range(pieces)
        for part in range(radix)
    ]
    constants = [
        pltpu.make_async_copy(source, to, constant_sems.at[i])
        for i, (source, to) in enumerate(zip(refs[:4], (taps, high, low, step)))
    ]
    for copy in constants + copies:
        copy.start()

    if kind == "all":
        dest_of = lambda item: item
    else:
        me = position(axes)
        dest_of = lambda item: me ^ within(axes, item)

    def store(item, c, chunk, part):
        for pol in range(pols):
            block = part[pol].astype(jnp.bfloat16)
            if kind == "near":
                out[item, 0, c, pol] = block
                out[item, 1, c, pol] = brought[item, c, pol]
            else:
                out[item, c, pol, :, pl.ds(chunk * CHUNK, CHUNK)] = block

    for copy in constants:
        copy.wait()
    fill_phases(high, low, phase)
    fill_table(0, dest_of, own, phase, step, table)
    steps = wide // LANES * pols

    def load(at_step, pol, part, at):
        for piece in range(pieces):
            pl.when(at_step == piece * steps)(copies[piece * radix + part].wait)
        if halo is not None:
            ext[part, pl.ds(0, ROWS), :] = halo[pol, :, at].astype(jnp.float32)
            ext[part, pl.ds(ROWS, held), :] = rows[pol, :, at].astype(jnp.float32)
        else:
            ext[part] = rows[pol, :, at].astype(jnp.float32)

    fir(load, count // CHUNK, taps, weighted, ext)
    transform(store, out.shape[0], dest_of, own, weighted, phase, step, (table, table_next), mixed)


def place_main_kernel(frames, block, held, out, sems):
    copies = []
    for source in range(block.shape[0]):
        at = pl.ds(source * frames, block.shape[4])
        copies.append(pltpu.make_async_copy(block.at[source], out.at[:, :, :, at], sems.at[source]))
    for copy in copies:
        copy.start()
    for copy in copies:
        copy.wait()


def place_near_kernel(axes, frames, begin, *refs):
    blocks, (mine, out, sems) = refs[:-3], refs[-3:]
    half = axes[1][1] // 2
    me = position(axes)
    copies = []
    for item in range(len(blocks) + 1):
        block = mine if item == 0 else blocks[item - 1]
        for side in range(2):
            source = me ^ (within(axes, item) + side * half)
            at = pl.ds(pl.multiple_of(source * frames + begin, CHUNK), frames - begin)
            copies.append(pltpu.make_async_copy(block.at[side], out.at[:, :, :, at], sems.at[2 * item + side]))
    for copy in copies:
        copy.start()
    for copy in copies:
        copy.wait()


def local(axes, samples, taps):
    pols, frames, nfft = samples.shape
    tap_count = taps.shape[0]
    channels = nfft // 2
    both = tuple(name for name, _ in axes)
    row_count, column_count = axes[0][1], axes[1][1]
    devices = row_count * column_count
    half = column_count // 2
    own = channels // devices
    chunks = frames // CHUNK
    radix = 2 if own % (nfft // LANES) == 0 else 1
    per = max(1, 256 * radix // (2 * own))
    assert own % ROWS == 0 and tap_count <= ROWS and nfft % (LANES * PIECES * radix) == 0 and frames % CHUNK == 0 and chunks > 1
    assert devices & (devices - 1) == 0 and half > 0 and row_count * half % (2 * per) == 0

    high, low, step = twiddles(nfft, radix)
    bf16 = jnp.bfloat16
    vmem = pl.BlockSpec(memory_space=pltpu.VMEM)
    anywhere = pl.BlockSpec(memory_space=pl.ANY)
    hbm = pl.BlockSpec(memory_space=pltpu.HBM)
    dma = pltpu.SemaphoreType.DMA
    nears = row_count * half
    begin = (chunks - LEAD) * CHUNK
    short = frames - begin

    fixed = [pltpu.with_memory_space_constraint(x, pltpu.HBM) for x in (samples, taps, high, low, step)]

    def compute(kind, at, count, shape, *extra):
        held = count * CHUNK + (0 if kind == "all" else ROWS)
        dests = devices if kind == "all" else nears
        return pl.pallas_call(
            functools.partial(compute_kernel, axes, kind, at, own),
            out_shape=(pltpu.HBM if kind == "all" else pltpu.VMEM)(shape, bf16),
            in_specs=[hbm] + [vmem] * len(extra) + [hbm] * 4,
            out_specs=vmem,
            scratch_shapes=[
                pltpu.VMEM((pols, held, nfft), bf16),
                pltpu.VMEM((radix, count, pols * CHUNK, nfft // radix), bf16),
                pltpu.VMEM((radix, count * CHUNK + ROWS, LANES), jnp.float32),
                pltpu.VMEM((2, channels, LANES), jnp.float32),
                pltpu.VMEM((radix, per * 2 * own // radix, nfft // radix), bf16),
                pltpu.VMEM((radix, per * 2 * own // radix, nfft // radix), bf16),
                pltpu.VMEM((pols * CHUNK // LANES, per * 2 * own, LANES), jnp.float32),
                pltpu.VMEM(taps.shape, taps.dtype),
                *(pltpu.VMEM(factor.shape, factor.dtype) for factor in (high, low, step)),
                dma((PIECES, radix)),
                dma((4,)),
            ],
            compiler_params=pltpu.CompilerParams(vmem_limit_bytes=VMEM_LIMIT),
            cost_estimate=pl.CostEstimate(
                flops=4 * dests * own * pols * count * CHUNK * nfft,
                bytes_accessed=2 * pols * count * CHUNK * nfft * 2,
                transcendentals=0,
            ),
        )(fixed[0], *extra, *fixed[1:])

    def swap(part, by):
        return lax.ppermute(part, both, [(i, i ^ by) for i in range(devices)])

    out_shape = jax.ShapeDtypeStruct((2, pols, own, devices * frames), bf16)
    small = pltpu.CompilerParams(vmem_limit_bytes=1024 * 1024)

    tables = (radix, per * 2 * own // radix, nfft // radix)
    tail, *ready = pl.pallas_call(
        functools.partial(prepare_kernel, axes, begin, own),
        out_shape=[
            pltpu.VMEM((pols, ROWS, nfft), bf16),
            pltpu.VMEM((pols, short + ROWS, nfft), bf16),
            pltpu.VMEM(taps.shape, taps.dtype),
            pltpu.VMEM(step.shape, step.dtype),
            pltpu.VMEM((2, channels, LANES), jnp.float32),
            pltpu.VMEM(tables, bf16),
        ],
        in_specs=[hbm] * 5,
        out_specs=[vmem] * 6,
        scratch_shapes=[pltpu.VMEM(high.shape, high.dtype), pltpu.VMEM(low.shape, low.dtype), dma((6,))],
        compiler_params=pltpu.CompilerParams(vmem_limit_bytes=VMEM_LIMIT),
        name="prepare",
    )(*fixed)
    halo = lax.ppermute(tail, both, [(i, i + 1) for i in range(devices - 1)])
    part = pl.pallas_call(
        functools.partial(far_kernel, axes, own),
        out_shape=pltpu.VMEM((nears, 2, pols, own, short), bf16),
        in_specs=[vmem] * 5,
        out_specs=vmem,
        scratch_shapes=[
            pltpu.VMEM((radix, LEAD, pols * CHUNK, nfft // radix), bf16),
            pltpu.VMEM((radix, short + ROWS, LANES), jnp.float32),
            pltpu.VMEM(tables, bf16),
            pltpu.VMEM(tables, bf16),
            pltpu.VMEM((pols * CHUNK // LANES, per * 2 * own, LANES), jnp.float32),
        ],
        compiler_params=pltpu.CompilerParams(vmem_limit_bytes=VMEM_LIMIT),
        cost_estimate=pl.CostEstimate(
            flops=4 * nears * own * pols * short * nfft, bytes_accessed=2 * pols * short * nfft * 2, transcendentals=0
        ),
        name="far",
    )(*[pltpu.with_memory_space_constraint(x, pltpu.VMEM) for x in ready])
    brought = swap(part, half)
    part = compute("all", 0, chunks - LEAD, (devices, 2, pols, own, begin), halo)
    arrived = lax.all_to_all(part, both, split_axis=0, concat_axis=0, tiled=True)
    part = compute("near", begin, LEAD, (nears, 2, 2, pols, own, short), brought)
    blocks = [swap(part[item], item // half * column_count + item % half) for item in range(1, nears)]
    out = pl.pallas_call(
        functools.partial(place_near_kernel, axes, frames, begin),
        out_shape=out_shape,
        in_specs=[anywhere] * (nears - 1) + [vmem],
        out_specs=anywhere,
        scratch_shapes=[dma((2 * nears,))],
        compiler_params=small,
        name="place_near",
    )(*blocks, part[0])
    return pl.pallas_call(
        functools.partial(place_main_kernel, frames),
        out_shape=out_shape,
        in_specs=[anywhere] * 2,
        out_specs=anywhere,
        scratch_shapes=[dma((devices,))],
        input_output_aliases={1: 0},
        compiler_params=small,
        name="place_main",
    )(arrived, out)


def solution(mesh):
    axes = tuple((name, mesh.shape[name]) for name in ("tm", "chan"))

    def body(samples, taps):
        return local(axes, samples, taps)

    return jax.shard_map(
        body,
        mesh=mesh,
        in_specs=(P(None, ("tm", "chan"), None), P()),
        out_specs=P(None, None, ("tm", "chan"), None),
        check_vma=False,
    )
```

```python
import functools

import jax
import jax.numpy as jnp
import numpy as np
from jax import lax
from jax.experimental import pallas as pl
from jax.experimental.pallas import tpu as pltpu
from jax.sharding import PartitionSpec as P


LANES = 128
ROWS = 8
CHUNK = 128
PIECES = 4
LEAD = 1
VMEM_LIMIT = 24 * 1024 * 1024


def twiddles(nfft, radix):
    span = nfft // LANES
    r = np.arange(span).reshape(-1, radix).T.reshape(-1)
    high = np.arange(nfft // 2 // span)[:, None] * span * np.arange(LANES)[None, :]
    low = r[:, None] * np.arange(LANES)[None, :]
    step = np.arange(span // radix)[:, None] * r[None, :] * LANES

    def pair(turns):
        angle = 2.0 * np.pi * (turns % nfft) / nfft
        return np.stack([np.cos(angle), np.sin(angle)]).astype(np.float32)

    step = np.broadcast_to(pair(step)[:, :, :, None] / 32.0, (2, span // radix, span, LANES))
    return jnp.asarray(pair(high)), jnp.asarray(pair(low)), jnp.asarray(np.ascontiguousarray(step))


def fir(load, chunks, taps_ref, weighted_ref, ext_ref):
    nfft = taps_ref.shape[1]
    tap_count = taps_ref.shape[0]
    radix = weighted_ref.shape[0]
    pols = weighted_ref.shape[2] // CHUNK
    width = nfft // radix
    rows = 64 // radix

    def body(step, carry):
        lane = pl.multiple_of(step * LANES, LANES)
        taps = []
        for part in range(radix):
            at = pl.ds(lane + part * width, LANES)
            load(step, part, at)
            taps.append(taps_ref[:, at])
        for chunk in range(chunks):
            for first in range(0, CHUNK, rows):
                for pol in range(pols):
                    totals = []
                    for part in range(radix):
                        total = None
                        for tap in range(tap_count):
                            start = ROWS + chunk * CHUNK + first + tap - (tap_count - 1)
                            term = taps[part][tap : tap + 1, :] * ext_ref[pol, part, pl.ds(start, rows), :]
                            total = term if total is None else total + term
                        totals.append(total)
                    to = pl.ds(pol * CHUNK + first, rows)
                    if radix == 2:
                        totals = [totals[0] + totals[1], totals[0] - totals[1]]
                    for part in range(radix):
                        weighted_ref[part, chunk, to, pl.ds(lane, LANES)] = totals[part].astype(jnp.bfloat16)
        return carry

    lax.fori_loop(0, width // LANES, body, 0)


def fill_phases(high_ref, low_ref, phase_ref):
    span = low_ref.shape[1]
    for a in range(high_ref.shape[1]):
        high_c, high_s = high_ref[0, pl.ds(a, 1), :], high_ref[1, pl.ds(a, 1), :]
        low_c, low_s = low_ref[0], low_ref[1]
        phase_ref[0, pl.ds(a * span, span), :] = high_c * low_c - high_s * low_s
        phase_ref[1, pl.ds(a * span, span), :] = -(high_s * low_c) - high_c * low_s


def fill_table(group, dest_of, own, phase_ref, step_ref, table_ref):
    radix = table_ref.shape[0]
    steps, span = step_ref.shape[1:3]
    per = table_ref.shape[1] * radix // (2 * own)
    height = min(own, span) // radix
    blocks = own * radix // (height * radix * radix)
    for slot in range(per):
        k = dest_of(group * per + slot) * own
        for part in range(radix):
            at = part * (span // radix)
            inner = 0 if height * radix == span else pl.multiple_of(lax.rem(k, span), ROWS)
            base = pl.multiple_of(k - inner, span)
            joined = lambda pieces: pieces[0] if len(pieces) == 1 else jnp.concatenate(pieces)
            rows = [pl.ds(pl.multiple_of(base + block * span + at + inner, ROWS), height) for block in range(blocks)]
            c = joined([phase_ref[0, r, :] for r in rows])
            s = joined([phase_ref[1, r, :] for r in rows])
            to_c = slot * 2 * own // radix
            to_s = to_c + own // radix
            for m in range(steps):
                of = pl.ds(pl.multiple_of(at + inner, ROWS), height)
                mc = joined([step_ref[0, m, of, :]] * blocks)
                ms = joined([step_ref[1, m, of, :]] * blocks)
                lanes = pl.ds(m * LANES, LANES)
                table_ref[part, pl.ds(to_c, own // radix), lanes] = (c * mc + s * ms).astype(jnp.bfloat16)
                table_ref[part, pl.ds(to_s, own // radix), lanes] = (s * mc - c * ms).astype(jnp.bfloat16)


def transform(store, count, dest_of, own, weighted_ref, phase_ref, step_ref, table_refs, mixed_ref):
    radix, rows, _ = table_refs[0].shape
    per = rows * radix // (2 * own)
    groups = count // per

    def one(group, now, later):
        for chunk in range(weighted_ref.shape[1]):
            for part in range(radix):
                found = lax.dot_general(
                    now[part],
                    weighted_ref[part, chunk],
                    (((1,), (1,)), ((), ())),
                    preferred_element_type=jnp.float32,
                )
                for side in range(mixed_ref.shape[0]):
                    to = pl.ds(part, rows, stride=radix) if radix > 1 else pl.ds(0, rows)
                    mixed_ref[side, to, :] = found[:, side * LANES : (side + 1) * LANES]
            for slot in range(per):
                for c in range(2):
                    row = pl.ds((slot * 2 + c) * own, own)
                    store(group * per + slot, c, chunk, [mixed_ref[side, row, :] for side in range(mixed_ref.shape[0])])
            if chunk == 0 and later is not None:
                fill_table(jnp.minimum(group + 1, groups - 1), dest_of, own, phase_ref, step_ref, later)

    def two(index, carry):
        one(2 * index, table_refs[0], table_refs[1])
        one(2 * index + 1, table_refs[1], table_refs[0])
        return carry

    if groups == 2:
        one(0, table_refs[0], table_refs[1])
        one(1, table_refs[1], None)
    else:
        lax.fori_loop(0, groups // 2, two, 0)


def position(axes):
    return lax.axis_index(axes[0][0]) * axes[1][1] + lax.axis_index(axes[1][0])


def within(axes, item):
    half = axes[1][1] // 2
    return item // half * axes[1][1] + item % half


def prepare_kernel(axes, begin, own, samples, taps, high, low, step, *refs):
    tail, rows, taps_out, step_out, phase, table, high_in, low_in, sems = refs
    frames = samples.shape[1]
    last = pl.ds(begin - ROWS, frames - begin + ROWS)
    moves = [
        (high, high_in),
        (low, low_in),
        (step, step_out),
        (samples.at[:, pl.ds(frames - ROWS, ROWS)], tail),
        (samples.at[:, last], rows),
        (taps, taps_out),
    ]
    copies = [pltpu.make_async_copy(source, to, sems.at[i]) for i, (source, to) in enumerate(moves)]
    for copy in copies:
        copy.start()
    for copy in copies[:3]:
        copy.wait()
    fill_phases(high_in, low_in, phase)
    me = position(axes)
    fill_table(0, lambda item: me ^ (within(axes, item) ^ (axes[1][1] - 1)), own, phase, step_out, table)
    for copy in copies[3:]:
        copy.wait()


def far_kernel(axes, own, rows, taps, step, phase, table, out, weighted, ext, table_next, table_spare, mixed):
    me = position(axes)
    dest_of = lambda item: me ^ (within(axes, item) ^ (axes[1][1] - 1))

    def load(at_step, part, at):
        ext[:, part] = rows[:, :, at].astype(jnp.float32)

    def store(item, c, chunk, part):
        for pol in range(out.shape[2]):
            out[item, c, pol, :, pl.ds(chunk * CHUNK, CHUNK)] = part[pol].astype(jnp.bfloat16)

    fir(load, weighted.shape[1], taps, weighted, ext)
    radix, height, _ = table.shape
    first = table
    if out.shape[0] != 2 * (height * radix // (2 * own)):
        table_spare[...] = table[...]
        first = table_spare
    transform(store, out.shape[0], dest_of, own, weighted, phase, step, (first, table_next), mixed)


def compute_kernel(axes, kind, begin, own, samples, *refs):
    refs = list(refs)
    halo = refs.pop(0) if kind == "all" else None
    brought = refs.pop(0) if kind == "near" else None
    out = refs[4]
    rows, weighted, ext, phase, table, table_next, mixed, taps, high, low, step, sems, constant_sems = refs[5:]
    pols, _, nfft = samples.shape
    radix = weighted.shape[0]
    count = weighted.shape[1] * CHUNK
    pieces = sems.shape[0]
    width = nfft // radix
    wide = width // pieces
    first = 0 if halo is not None else begin - ROWS
    held = begin + count - first
    copies = [
        pltpu.make_async_copy(
            samples.at[:, pl.ds(first, held), pl.ds(part * width + piece * wide, wide)],
            rows.at[:, :, pl.ds(part * width + piece * wide, wide)],
            sems.at[piece, part],
        )
        for piece in range(pieces)
        for part in range(radix)
    ]
    constants = [
        pltpu.make_async_copy(source, to, constant_sems.at[i])
        for i, (source, to) in enumerate(zip(refs[:4], (taps, high, low, step)))
    ]
    for copy in constants + copies:
        copy.start()

    if kind == "all":
        dest_of = lambda item: item
    else:
        me = position(axes)
        dest_of = lambda item: me ^ within(axes, item)

    def store(item, c, chunk, part):
        for pol in range(pols):
            block = part[pol].astype(jnp.bfloat16)
            if kind == "near":
                out[item, 0, c, pol] = block
                out[item, 1, c, pol] = brought[item, c, pol]
            else:
                out[item, c, pol, :, pl.ds(chunk * CHUNK, CHUNK)] = block

    for copy in constants:
        copy.wait()
    fill_phases(high, low, phase)
    fill_table(0, dest_of, own, phase, step, table)
    steps = wide // LANES

    def load(at_step, part, at):
        for piece in range(pieces):
            pl.when(at_step == piece * steps)(copies[piece * radix + part].wait)
        if halo is not None:
            ext[:, part, pl.ds(0, ROWS), :] = halo[:, :, at].astype(jnp.float32)
            ext[:, part, pl.ds(ROWS, held), :] = rows[:, :, at].astype(jnp.float32)
        else:
            ext[:, part] = rows[:, :, at].astype(jnp.float32)

    fir(load, count // CHUNK, taps, weighted, ext)
    transform(store, out.shape[0], dest_of, own, weighted, phase, step, (table, table_next), mixed)


def place_main_kernel(frames, block, held, out, sems):
    copies = []
    for source in range(block.shape[0]):
        at = pl.ds(source * frames, block.shape[4])
        copies.append(pltpu.make_async_copy(block.at[source], out.at[:, :, :, at], sems.at[source]))
    for copy in copies:
        copy.start()
    for copy in copies:
        copy.wait()


def place_near_kernel(axes, frames, begin, *refs):
    blocks, (mine, out, sems) = refs[:-3], refs[-3:]
    me = position(axes)
    copies = []
    for item in range(len(blocks) + 1):
        block = mine if item == 0 else blocks[item - 1]
        for side in range(2):
            source = me ^ (within(axes, item) ^ (side * (axes[1][1] - 1)))
            at = pl.ds(pl.multiple_of(source * frames + begin, CHUNK), frames - begin)
            copies.append(pltpu.make_async_copy(block.at[side], out.at[:, :, :, at], sems.at[2 * item + side]))
    for copy in copies:
        copy.start()
    for copy in copies:
        copy.wait()


def local(axes, samples, taps):
    pols, frames, nfft = samples.shape
    tap_count = taps.shape[0]
    channels = nfft // 2
    both = tuple(name for name, _ in axes)
    row_count, column_count = axes[0][1], axes[1][1]
    devices = row_count * column_count
    half = column_count // 2
    own = channels // devices
    chunks = frames // CHUNK
    radix = 2 if own % (nfft // LANES) == 0 else 1
    per = max(1, 256 * radix // (2 * own))
    assert own % ROWS == 0 and tap_count <= ROWS and nfft % (LANES * PIECES * radix) == 0 and frames % CHUNK == 0 and chunks > 1
    assert devices & (devices - 1) == 0 and half > 0 and row_count * half % (2 * per) == 0

    high, low, step = twiddles(nfft, radix)
    bf16 = jnp.bfloat16
    vmem = pl.BlockSpec(memory_space=pltpu.VMEM)
    anywhere = pl.BlockSpec(memory_space=pl.ANY)
    hbm = pl.BlockSpec(memory_space=pltpu.HBM)
    dma = pltpu.SemaphoreType.DMA
    nears = row_count * half
    begin = (chunks - LEAD) * CHUNK
    short = frames - begin

    fixed = [pltpu.with_memory_space_constraint(x, pltpu.HBM) for x in (samples, taps, high, low, step)]

    def compute(kind, at, count, shape, *extra):
        held = count * CHUNK + (0 if kind == "all" else ROWS)
        dests = devices if kind == "all" else nears
        return pl.pallas_call(
            functools.partial(compute_kernel, axes, kind, at, own),
            out_shape=(pltpu.HBM if kind == "all" else pltpu.VMEM)(shape, bf16),
            in_specs=[hbm] + [vmem] * len(extra) + [hbm] * 4,
            out_specs=vmem,
            scratch_shapes=[
                pltpu.VMEM((pols, held, nfft), bf16),
                pltpu.VMEM((radix, count, pols * CHUNK, nfft // radix), bf16),
                pltpu.VMEM((pols, radix, count * CHUNK + ROWS, LANES), jnp.float32),
                pltpu.VMEM((2, channels, LANES), jnp.float32),
                pltpu.VMEM((radix, per * 2 * own // radix, nfft // radix), bf16),
                pltpu.VMEM((radix, per * 2 * own // radix, nfft // radix), bf16),
                pltpu.VMEM((pols * CHUNK // LANES, per * 2 * own, LANES), jnp.float32),
                pltpu.VMEM(taps.shape, taps.dtype),
                *(pltpu.VMEM(factor.shape, factor.dtype) for factor in (high, low, step)),
                dma((PIECES, radix)),
                dma((4,)),
            ],
            compiler_params=pltpu.CompilerParams(vmem_limit_bytes=VMEM_LIMIT),
            cost_estimate=pl.CostEstimate(
                flops=4 * dests * own * pols * count * CHUNK * nfft,
                bytes_accessed=2 * pols * count * CHUNK * nfft * 2,
                transcendentals=0,
            ),
        )(fixed[0], *extra, *fixed[1:])

    def swap(part, by):
        return lax.ppermute(part, both, [(i, i ^ by) for i in range(devices)])

    out_shape = jax.ShapeDtypeStruct((2, pols, own, devices * frames), bf16)
    small = pltpu.CompilerParams(vmem_limit_bytes=1024 * 1024)

    tables = (radix, per * 2 * own // radix, nfft // radix)
    tail, *ready = pl.pallas_call(
        functools.partial(prepare_kernel, axes, begin, own),
        out_shape=[
            pltpu.VMEM((pols, ROWS, nfft), bf16),
            pltpu.VMEM((pols, short + ROWS, nfft), bf16),
            pltpu.VMEM(taps.shape, taps.dtype),
            pltpu.VMEM(step.shape, step.dtype),
            pltpu.VMEM((2, channels, LANES), jnp.float32),
            pltpu.VMEM(tables, bf16),
        ],
        in_specs=[hbm] * 5,
        out_specs=[vmem] * 6,
        scratch_shapes=[pltpu.VMEM(high.shape, high.dtype), pltpu.VMEM(low.shape, low.dtype), dma((6,))],
        compiler_params=pltpu.CompilerParams(vmem_limit_bytes=VMEM_LIMIT),
        name="prepare",
    )(*fixed)
    halo = lax.ppermute(tail, both, [(i, i + 1) for i in range(devices - 1)])
    part = pl.pallas_call(
        functools.partial(far_kernel, axes, own),
        out_shape=pltpu.VMEM((nears, 2, pols, own, short), bf16),
        in_specs=[vmem] * 5,
        out_specs=vmem,
        scratch_shapes=[
            pltpu.VMEM((radix, LEAD, pols * CHUNK, nfft // radix), bf16),
            pltpu.VMEM((pols, radix, short + ROWS, LANES), jnp.float32),
            pltpu.VMEM(tables, bf16),
            pltpu.VMEM(tables, bf16),
            pltpu.VMEM((pols * CHUNK // LANES, per * 2 * own, LANES), jnp.float32),
        ],
        compiler_params=pltpu.CompilerParams(vmem_limit_bytes=VMEM_LIMIT),
        cost_estimate=pl.CostEstimate(
            flops=4 * nears * own * pols * short * nfft, bytes_accessed=2 * pols * short * nfft * 2, transcendentals=0
        ),
        name="far",
    )(*[pltpu.with_memory_space_constraint(x, pltpu.VMEM) for x in ready])
    brought = swap(part, column_count - 1)
    part = compute("all", 0, chunks - LEAD, (devices, 2, pols, own, begin), halo)
    arrived = lax.all_to_all(part, both, split_axis=0, concat_axis=0, tiled=True)
    part = compute("near", begin, LEAD, (nears, 2, 2, pols, own, short), brought)
    blocks = [swap(part[item], item // half * column_count + item % half) for item in range(1, nears)]
    out = pl.pallas_call(
        functools.partial(place_near_kernel, axes, frames, begin),
        out_shape=out_shape,
        in_specs=[anywhere] * (nears - 1) + [vmem],
        out_specs=anywhere,
        scratch_shapes=[dma((2 * nears,))],
        compiler_params=small,
        name="place_near",
    )(*blocks, part[0])
    return pl.pallas_call(
        functools.partial(place_main_kernel, frames),
        out_shape=out_shape,
        in_specs=[anywhere] * 2,
        out_specs=anywhere,
        scratch_shapes=[dma((devices,))],
        input_output_aliases={1: 0},
        compiler_params=small,
        name="place_main",
    )(arrived, out)


def solution(mesh):
    axes = tuple((name, mesh.shape[name]) for name in ("tm", "chan"))

    def body(samples, taps):
        return local(axes, samples, taps)

    return jax.shard_map(
        body,
        mesh=mesh,
        in_specs=(P(None, ("tm", "chan"), None), P()),
        out_specs=P(None, None, ("tm", "chan"), None),
        check_vma=False,
    )
```

```python
import functools

import jax
import jax.numpy as jnp
import numpy as np
from jax import lax
from jax.experimental import pallas as pl
from jax.experimental.pallas import tpu as pltpu
from jax.sharding import PartitionSpec as P


LANES = 128
ROWS = 8
CHUNK = 128
PIECES = 4
LEAD = 1
VMEM_LIMIT = 24 * 1024 * 1024


def twiddles(nfft, radix):
    span = nfft // LANES
    r = np.arange(span).reshape(-1, radix).T.reshape(-1)
    high = np.arange(nfft // 2 // span)[:, None] * span * np.arange(LANES)[None, :]
    low = r[:, None] * np.arange(LANES)[None, :]
    step = np.arange(span // radix)[:, None] * r[None, :] * LANES

    def pair(turns):
        angle = 2.0 * np.pi * (turns % nfft) / nfft
        return np.stack([np.cos(angle), np.sin(angle)]).astype(np.float32)

    step = np.broadcast_to(pair(step)[:, :, :, None] / 32.0, (2, span // radix, span, LANES))
    return jnp.asarray(pair(high)), jnp.asarray(pair(low)), jnp.asarray(np.ascontiguousarray(step))


def fir(load, chunks, taps_ref, weighted_ref, ext_ref):
    nfft = taps_ref.shape[1]
    tap_count = taps_ref.shape[0]
    radix = weighted_ref.shape[0]
    pols = weighted_ref.shape[2] // CHUNK
    width = nfft // radix
    rows = 64 // radix

    def body(step, carry):
        lane = pl.multiple_of(step * LANES, LANES)
        taps = []
        for part in range(radix):
            at = pl.ds(lane + part * width, LANES)
            load(step, part, at)
            taps.append(taps_ref[:, at])
        for chunk in range(chunks):
            for first in range(0, CHUNK, rows):
                for pol in range(pols):
                    totals = []
                    for part in range(radix):
                        total = None
                        for tap in range(tap_count):
                            start = ROWS + chunk * CHUNK + first + tap - (tap_count - 1)
                            term = taps[part][tap : tap + 1, :] * ext_ref[pol, part, pl.ds(start, rows), :]
                            total = term if total is None else total + term
                        totals.append(total)
                    to = pl.ds(pol * CHUNK + first, rows)
                    if radix == 2:
                        totals = [totals[0] + totals[1], totals[0] - totals[1]]
                    for part in range(radix):
                        weighted_ref[part, chunk, to, pl.ds(lane, LANES)] = totals[part].astype(jnp.bfloat16)
        return carry

    lax.fori_loop(0, width // LANES, body, 0)


def fill_phases(high_ref, low_ref, phase_ref):
    span = low_ref.shape[1]
    for a in range(high_ref.shape[1]):
        high_c, high_s = high_ref[0, pl.ds(a, 1), :], high_ref[1, pl.ds(a, 1), :]
        low_c, low_s = low_ref[0], low_ref[1]
        phase_ref[0, pl.ds(a * span, span), :] = high_c * low_c - high_s * low_s
        phase_ref[1, pl.ds(a * span, span), :] = -(high_s * low_c) - high_c * low_s


def fill_table(group, dest_of, own, phase_ref, step_ref, table_ref):
    radix = table_ref.shape[0]
    steps, span = step_ref.shape[1:3]
    per = table_ref.shape[1] * radix // (2 * own)
    height = min(own, span) // radix
    blocks = own * radix // (height * radix * radix)
    for slot in range(per):
        k = dest_of(group * per + slot) * own
        for part in range(radix):
            at = part * (span // radix)
            inner = 0 if height * radix == span else pl.multiple_of(lax.rem(k, span), ROWS)
            base = pl.multiple_of(k - inner, span)
            joined = lambda pieces: pieces[0] if len(pieces) == 1 else jnp.concatenate(pieces)
            rows = [pl.ds(pl.multiple_of(base + block * span + at + inner, ROWS), height) for block in range(blocks)]
            c = joined([phase_ref[0, r, :] for r in rows])
            s = joined([phase_ref[1, r, :] for r in rows])
            to_c = slot * 2 * own // radix
            to_s = to_c + own // radix
            for m in range(steps):
                of = pl.ds(pl.multiple_of(at + inner, ROWS), height)
                mc = joined([step_ref[0, m, of, :]] * blocks)
                ms = joined([step_ref[1, m, of, :]] * blocks)
                lanes = pl.ds(m * LANES, LANES)
                table_ref[part, pl.ds(to_c, own // radix), lanes] = (c * mc + s * ms).astype(jnp.bfloat16)
                table_ref[part, pl.ds(to_s, own // radix), lanes] = (s * mc - c * ms).astype(jnp.bfloat16)


def transform(store, count, dest_of, own, weighted_ref, phase_ref, step_ref, table_refs, mixed_ref):
    radix, rows, _ = table_refs[0].shape
    per = rows * radix // (2 * own)
    groups = count // per

    def one(group, now, later):
        for chunk in range(weighted_ref.shape[1]):
            for part in range(radix):
                found = lax.dot_general(
                    now[part],
                    weighted_ref[part, chunk],
                    (((1,), (1,)), ((), ())),
                    preferred_element_type=jnp.float32,
                )
                for side in range(mixed_ref.shape[0]):
                    to = pl.ds(part, rows, stride=radix) if radix > 1 else pl.ds(0, rows)
                    mixed_ref[side, to, :] = found[:, side * LANES : (side + 1) * LANES]
            for slot in range(per):
                for c in range(2):
                    row = pl.ds((slot * 2 + c) * own, own)
                    store(group * per + slot, c, chunk, [mixed_ref[side, row, :] for side in range(mixed_ref.shape[0])])
            if chunk == 0 and later is not None:
                fill_table(jnp.minimum(group + 1, groups - 1), dest_of, own, phase_ref, step_ref, later)

    def two(index, carry):
        one(2 * index, table_refs[0], table_refs[1])
        one(2 * index + 1, table_refs[1], table_refs[0])
        return carry

    if groups == 2:
        one(0, table_refs[0], table_refs[1])
        one(1, table_refs[1], None)
    else:
        lax.fori_loop(0, groups // 2, two, 0)


def position(axes):
    return lax.axis_index(axes[0][0]) * axes[1][1] + lax.axis_index(axes[1][0])


def within(axes, item):
    half = axes[1][1] // 2
    return item // half * axes[1][1] + item % half


def prepare_kernel(axes, begin, own, samples, taps, high, low, step, *refs):
    tail, rows, taps_out, step_out, phase, table, high_in, low_in, sems = refs
    frames = samples.shape[1]
    held = frames - begin + ROWS
    cut = held // 2 // ROWS * ROWS
    spans = [(pol, start, size) for pol in range(samples.shape[0]) for start, size in ((0, cut), (cut, held - cut))]
    moves = [
        (high, high_in),
        (low, low_in),
        (step, step_out),
        (samples.at[:, pl.ds(frames - ROWS, ROWS)], tail),
        (taps, taps_out),
        *(
            (samples.at[pol, pl.ds(begin - ROWS + start, size)], rows.at[pol, pl.ds(start, size)])
            for pol, start, size in spans
        ),
    ]
    copies = [pltpu.make_async_copy(source, to, sems.at[i]) for i, (source, to) in enumerate(moves)]
    for copy in copies:
        copy.start()
    for copy in copies[:3]:
        copy.wait()
    fill_phases(high_in, low_in, phase)
    me = position(axes)
    fill_table(0, lambda item: me ^ (within(axes, item) ^ (axes[1][1] - 1)), own, phase, step_out, table)
    for copy in copies[3:]:
        copy.wait()


def far_kernel(axes, own, rows, taps, step, phase, table, out, weighted, ext, table_next, table_spare, mixed):
    me = position(axes)
    dest_of = lambda item: me ^ (within(axes, item) ^ (axes[1][1] - 1))

    def load(at_step, part, at):
        ext[:, part] = rows[:, :, at].astype(jnp.float32)

    def store(item, c, chunk, part):
        for pol in range(out.shape[2]):
            out[item, c, pol, :, pl.ds(chunk * CHUNK, CHUNK)] = part[pol].astype(jnp.bfloat16)

    fir(load, weighted.shape[1], taps, weighted, ext)
    radix, height, _ = table.shape
    first = table
    if out.shape[0] != 2 * (height * radix // (2 * own)):
        table_spare[...] = table[...]
        first = table_spare
    transform(store, out.shape[0], dest_of, own, weighted, phase, step, (first, table_next), mixed)


def compute_kernel(axes, kind, begin, own, samples, *refs):
    refs = list(refs)
    halo = refs.pop(0) if kind == "all" else None
    brought = refs.pop(0) if kind == "near" else None
    out = refs[4]
    rows, weighted, ext, phase, table, table_next, mixed, taps, high, low, step, sems, constant_sems = refs[5:]
    pols, _, nfft = samples.shape
    radix = weighted.shape[0]
    count = weighted.shape[1] * CHUNK
    pieces = sems.shape[0]
    width = nfft // radix
    wide = width // pieces
    first = 0 if halo is not None else begin - ROWS
    held = begin + count - first
    copies = [
        pltpu.make_async_copy(
            samples.at[:, pl.ds(first, held), pl.ds(part * width + piece * wide, wide)],
            rows.at[:, :, pl.ds(part * width + piece * wide, wide)],
            sems.at[piece, part],
        )
        for piece in range(pieces)
        for part in range(radix)
    ]
    constants = [
        pltpu.make_async_copy(source, to, constant_sems.at[i])
        for i, (source, to) in enumerate(zip(refs[:4], (taps, high, low, step)))
    ]
    for copy in constants + copies:
        copy.start()

    if kind == "all":
        dest_of = lambda item: item
    else:
        me = position(axes)
        dest_of = lambda item: me ^ within(axes, item)

    def store(item, c, chunk, part):
        for pol in range(pols):
            block = part[pol].astype(jnp.bfloat16)
            if kind == "near":
                out[item, 0, c, pol] = block
                out[item, 1, c, pol] = brought[item, c, pol]
            else:
                out[item, c, pol, :, pl.ds(chunk * CHUNK, CHUNK)] = block

    for copy in constants:
        copy.wait()
    fill_phases(high, low, phase)
    fill_table(0, dest_of, own, phase, step, table)
    steps = wide // LANES

    def load(at_step, part, at):
        for piece in range(pieces):
            pl.when(at_step == piece * steps)(copies[piece * radix + part].wait)
        if halo is not None:
            ext[:, part, pl.ds(0, ROWS), :] = halo[:, :, at].astype(jnp.float32)
            ext[:, part, pl.ds(ROWS, held), :] = rows[:, :, at].astype(jnp.float32)
        else:
            ext[:, part] = rows[:, :, at].astype(jnp.float32)

    fir(load, count // CHUNK, taps, weighted, ext)
    transform(store, out.shape[0], dest_of, own, weighted, phase, step, (table, table_next), mixed)


def place_main_kernel(frames, block, held, out, sems):
    copies = []
    for source in range(block.shape[0]):
        at = pl.ds(source * frames, block.shape[4])
        copies.append(pltpu.make_async_copy(block.at[source], out.at[:, :, :, at], sems.at[source]))
    for copy in copies:
        copy.start()
    for copy in copies:
        copy.wait()


def place_near_kernel(axes, frames, begin, *refs):
    blocks, (mine, out, sems) = refs[:-3], refs[-3:]
    me = position(axes)
    copies = []
    for item in range(len(blocks) + 1):
        block = mine if item == 0 else blocks[item - 1]
        for side in range(2):
            source = me ^ (within(axes, item) ^ (side * (axes[1][1] - 1)))
            at = pl.ds(pl.multiple_of(source * frames + begin, CHUNK), frames - begin)
            copies.append(pltpu.make_async_copy(block.at[side], out.at[:, :, :, at], sems.at[2 * item + side]))
    for copy in copies:
        copy.start()
    for copy in copies:
        copy.wait()


def local(axes, samples, taps):
    pols, frames, nfft = samples.shape
    tap_count = taps.shape[0]
    channels = nfft // 2
    both = tuple(name for name, _ in axes)
    row_count, column_count = axes[0][1], axes[1][1]
    devices = row_count * column_count
    half = column_count // 2
    own = channels // devices
    chunks = frames // CHUNK
    radix = 2 if own % (nfft // LANES) == 0 else 1
    per = max(1, 256 * radix // (2 * own))
    assert own % ROWS == 0 and tap_count <= ROWS and nfft % (LANES * PIECES * radix) == 0 and frames % CHUNK == 0 and chunks > 1
    assert devices & (devices - 1) == 0 and half > 0 and row_count * half % (2 * per) == 0

    high, low, step = twiddles(nfft, radix)
    bf16 = jnp.bfloat16
    vmem = pl.BlockSpec(memory_space=pltpu.VMEM)
    anywhere = pl.BlockSpec(memory_space=pl.ANY)
    hbm = pl.BlockSpec(memory_space=pltpu.HBM)
    dma = pltpu.SemaphoreType.DMA
    nears = row_count * half
    begin = (chunks - LEAD) * CHUNK
    short = frames - begin

    fixed = [pltpu.with_memory_space_constraint(x, pltpu.HBM) for x in (samples, taps, high, low, step)]

    def compute(kind, at, count, shape, *extra):
        held = count * CHUNK + (0 if kind == "all" else ROWS)
        dests = devices if kind == "all" else nears
        return pl.pallas_call(
            functools.partial(compute_kernel, axes, kind, at, own),
            out_shape=(pltpu.HBM if kind == "all" else pltpu.VMEM)(shape, bf16),
            in_specs=[hbm] + [vmem] * len(extra) + [hbm] * 4,
            out_specs=vmem,
            scratch_shapes=[
                pltpu.VMEM((pols, held, nfft), bf16),
                pltpu.VMEM((radix, count, pols * CHUNK, nfft // radix), bf16),
                pltpu.VMEM((pols, radix, count * CHUNK + ROWS, LANES), jnp.float32),
                pltpu.VMEM((2, channels, LANES), jnp.float32),
                pltpu.VMEM((radix, per * 2 * own // radix, nfft // radix), bf16),
                pltpu.VMEM((radix, per * 2 * own // radix, nfft // radix), bf16),
                pltpu.VMEM((pols * CHUNK // LANES, per * 2 * own, LANES), jnp.float32),
                pltpu.VMEM(taps.shape, taps.dtype),
                *(pltpu.VMEM(factor.shape, factor.dtype) for factor in (high, low, step)),
                dma((PIECES, radix)),
                dma((4,)),
            ],
            compiler_params=pltpu.CompilerParams(vmem_limit_bytes=VMEM_LIMIT),
            cost_estimate=pl.CostEstimate(
                flops=4 * dests * own * pols * count * CHUNK * nfft,
                bytes_accessed=2 * pols * count * CHUNK * nfft * 2,
                transcendentals=0,
            ),
        )(fixed[0], *extra, *fixed[1:])

    def swap(part, by):
        return lax.ppermute(part, both, [(i, i ^ by) for i in range(devices)])

    out_shape = jax.ShapeDtypeStruct((2, pols, own, devices * frames), bf16)
    small = pltpu.CompilerParams(vmem_limit_bytes=1024 * 1024)

    tables = (radix, per * 2 * own // radix, nfft // radix)
    tail, *ready = pl.pallas_call(
        functools.partial(prepare_kernel, axes, begin, own),
        out_shape=[
            pltpu.VMEM((pols, ROWS, nfft), bf16),
            pltpu.VMEM((pols, short + ROWS, nfft), bf16),
            pltpu.VMEM(taps.shape, taps.dtype),
            pltpu.VMEM(step.shape, step.dtype),
            pltpu.VMEM((2, channels, LANES), jnp.float32),
            pltpu.VMEM(tables, bf16),
        ],
        in_specs=[hbm] * 5,
        out_specs=[vmem] * 6,
        scratch_shapes=[pltpu.VMEM(high.shape, high.dtype), pltpu.VMEM(low.shape, low.dtype), dma((5 + 2 * pols,))],
        compiler_params=pltpu.CompilerParams(vmem_limit_bytes=VMEM_LIMIT),
        name="prepare",
    )(*fixed)
    halo = lax.ppermute(tail, both, [(i, i + 1) for i in range(devices - 1)])
    part = pl.pallas_call(
        functools.partial(far_kernel, axes, own),
        out_shape=pltpu.VMEM((nears, 2, pols, own, short), bf16),
        in_specs=[vmem] * 5,
        out_specs=vmem,
        scratch_shapes=[
            pltpu.VMEM((radix, LEAD, pols * CHUNK, nfft // radix), bf16),
            pltpu.VMEM((pols, radix, short + ROWS, LANES), jnp.float32),
            pltpu.VMEM(tables, bf16),
            pltpu.VMEM(tables, bf16),
            pltpu.VMEM((pols * CHUNK // LANES, per * 2 * own, LANES), jnp.float32),
        ],
        compiler_params=pltpu.CompilerParams(vmem_limit_bytes=VMEM_LIMIT),
        cost_estimate=pl.CostEstimate(
            flops=4 * nears * own * pols * short * nfft, bytes_accessed=2 * pols * short * nfft * 2, transcendentals=0
        ),
        name="far",
    )(*[pltpu.with_memory_space_constraint(x, pltpu.VMEM) for x in ready])
    brought = swap(part, column_count - 1)
    part = compute("all", 0, chunks - LEAD, (devices, 2, pols, own, begin), halo)
    arrived = lax.all_to_all(part, both, split_axis=0, concat_axis=0, tiled=True)
    part = compute("near", begin, LEAD, (nears, 2, 2, pols, own, short), brought)
    blocks = [swap(part[item], item // half * column_count + item % half) for item in range(1, nears)]
    out = pl.pallas_call(
        functools.partial(place_near_kernel, axes, frames, begin),
        out_shape=out_shape,
        in_specs=[anywhere] * (nears - 1) + [vmem],
        out_specs=anywhere,
        scratch_shapes=[dma((2 * nears,))],
        compiler_params=small,
        name="place_near",
    )(*blocks, part[0])
    return pl.pallas_call(
        functools.partial(place_main_kernel, frames),
        out_shape=out_shape,
        in_specs=[anywhere] * 2,
        out_specs=anywhere,
        scratch_shapes=[dma((devices,))],
        input_output_aliases={1: 0},
        compiler_params=small,
        name="place_main",
    )(arrived, out)


def solution(mesh):
    axes = tuple((name, mesh.shape[name]) for name in ("tm", "chan"))

    def body(samples, taps):
        return local(axes, samples, taps)

    return jax.shard_map(
        body,
        mesh=mesh,
        in_specs=(P(None, ("tm", "chan"), None), P()),
        out_specs=P(None, None, ("tm", "chan"), None),
        check_vma=False,
    )
```
